256 devices in a mesh: gx: 64 (over y, x_lo, z), gy: 4 (over x_hi, core).
Axes of the slice: x: 4 (x_hi: 2, x_lo: 2; x = x_hi * 2 + x_lo), y: 4, z: 8, core: 2. Of those that a mesh axis runs over, the one named last changes fastest.
Arguments:
- positions: float32 [3, 128, 8, 256], P(None, 'gx', 'gy'), may hold values from 0 to 16, as said below
- velocities: float32 [3, 128, 8, 256], P(None, 'gx', 'gy'), may hold values from -3 to 3
- occupancy: int32 [128, 8], P('gx', 'gy'), may hold values from 64 to 256
- cot_positions: float32 [3, 128, 8, 256], P(None, 'gx', 'gy'), may hold values from -6 to 6
- cot_velocities: float32 [3, 128, 8, 256], P(None, 'gx', 'gy'), may hold values from -6 to 6
Outputs:
- grad_positions: float32 [3, 128, 8, 256], P(None, 'gx', 'gy')
- grad_velocities: float32 [3, 128, 8, 256], P(None, 'gx', 'gy')
The draws below stay inside these ranges and needn't reach their ends.
Inputs may be any that keep to these rules, and one draw needn't show every extreme that they name: `positions`: components 0 and 1 lie in [0, 1), the offset in the tile's cell; component 2 lies in [0, 16). Slots 0 to occupancy - 1 of a tile hold particles, the other slots are empty.
All inputs are finite; a program needn't handle non-finite values.
Results may differ from the reference program's by a relative error of at most 0.0003.
Values sent between devices are 32-bit elements; how exact they have to be, the bound alone decides.
A program may use at most 128 MiB of HBM per device.

```python
import jax
import jax.numpy as jnp
from jax import lax

P_SIZE = 256
ZH = 16
TX = 2
STEPS = 4
TXG = 128
TYG = 8


def draw_positions(key, part):
    uniform_draw = jax.random.uniform(key, (3, TXG, TYG, P_SIZE), jnp.float32)
    scales = jnp.array([1.0, 1.0, float(ZH)], jnp.float32)[:, None, None, None]
    return uniform_draw * scales


def with_ends(values, stream_key, low, top_value):
    extent = values.shape
    spot = [jax.random.randint(jax.random.fold_in(stream_key, axis), (), 0, extent[axis]) for axis in range(len(extent))]
    values = values.at[tuple(spot)].set(low)
    longest = extent.index(max(extent))
    spot[longest] = (spot[longest] + 1) % extent[longest]
    return values.at[tuple(spot)].set(top_value)


def level_of(rng, dims, cuts, smallest, top_value):
    level = 1.0
    for axis_at, blocks in cuts:
        heights = jax.random.uniform(jax.random.fold_in(jax.random.fold_in(rng, 6), axis_at), (blocks,), jnp.float32, smallest / len(cuts), top_value / len(cuts))
        level = level * jnp.repeat(jnp.exp(heights), dims[axis_at] // blocks).reshape((-1,) + (1,) * (len(dims) - 1 - axis_at))
    return level


def gaussian(stream_key, dims, spread, bound, split=(), kind=jnp.bfloat16):
    drawn = spread * jax.random.normal(stream_key, dims, jnp.float32)
    if split:
        drawn = drawn * level_of(stream_key, dims, split, -0.22, 0.18)
    return jnp.clip(drawn, -bound, bound).astype(kind)


def setup_inputs(seed: int = 0) -> dict:
    key_of = jax.random.split(jax.random.key(seed), 6)
    return {
        "positions": draw_positions(jax.random.fold_in(key_of[5], 71), 0),
        "velocities": gaussian(key_of[1], (3, TXG, TYG, P_SIZE), 0.5, 3.0, ((1, 64), (2, 4)), jnp.float32),
        "occupancy": with_ends(jax.random.randint(key_of[2], (TXG, TYG), P_SIZE // 4, P_SIZE + 1), jax.random.fold_in(key_of[2], 1), P_SIZE // 4, P_SIZE).astype(jnp.int32),
        "cot_positions": gaussian(key_of[3], (3, TXG, TYG, P_SIZE), 1.0, 6.0, ((1, 64), (2, 4)), jnp.float32),
        "cot_velocities": gaussian(key_of[4], (3, TXG, TYG, P_SIZE), 1.0, 6.0, ((1, 64), (2, 4)), jnp.float32),
    }


time_step = 0.05
stiffness = 4.0
rest_density = 1.0
particle_mass = 0.15
viscosity = 0.5
stencil = ((-1, -1), (-1, 0), (-1, 1), (0, -1), (0, 0), (0, 1), (1, -1), (1, 0), (1, 1))

def separation(middle_tile, nearby, displace_x, displace_y):
    offsets = (float(displace_x), float(displace_y), 0.0)
    return [nearby[coord_id][..., None, :] - middle_tile[coord_id][..., :, None] + offsets[coord_id] for coord_id in range(3)]

def intersection_of(pieces):
    return jnp.maximum(1.0 - (pieces[0] * pieces[0] + pieces[1] * pieces[1] + pieces[2] * pieces[2]), 0.0)

def pairwise_density(middle_tile, nearby, displace_x, displace_y):
    intersection = intersection_of(separation(middle_tile, nearby, displace_x, displace_y))
    masses = particle_mass * nearby[3][..., None, :]
    return lax.optimization_barrier(jnp.sum(masses * intersection * intersection * intersection, axis=-1))[None]

def accel_pairs(middle_tile, nearby, displace_x, displace_y):
    pieces = separation(middle_tile, nearby, displace_x, displace_y)
    intersection = intersection_of(pieces)
    masses = particle_mass * nearby[6][..., None, :]
    pressure_push = 6.0 * masses * (middle_tile[6][..., :, None] + nearby[7][..., None, :]) * intersection * intersection
    viscous = viscosity * masses * nearby[8][..., None, :] * intersection * intersection * intersection
    components = [lax.optimization_barrier(jnp.sum(viscous * (nearby[3 + coord_id][..., None, :] - middle_tile[3 + coord_id][..., :, None]) - pressure_push * pieces[coord_id], axis=-1)) for coord_id in range(3)]
    return jnp.stack(components)

def adjacent_tiles(field, displace_x, displace_y):
    rolled = jnp.roll(field, -displace_x, axis=1)
    if displace_y == 1:
        rolled = jnp.concatenate([rolled[:, :, 1:], jnp.zeros_like(rolled[:, :, :1])], axis=2)
    if displace_y == -1:
        rolled = jnp.concatenate([jnp.zeros_like(rolled[:, :, :1]), rolled[:, :, :-1]], axis=2)
    return rolled

def grouped_by_block(pair_fn, middle_tile, nearby, displace_x, displace_y):
    nblocks = middle_tile.shape[1] // TX

    def to_blocks(field):
        return jnp.moveaxis(field.reshape(field.shape[0], nblocks, TX, field.shape[2], field.shape[3]), 1, 0)
    checked = jax.checkpoint(pair_fn, static_argnums=(2, 3))

    def block_pairs(block_args):
        return checked(block_args[0], block_args[1], displace_x, displace_y)
    result = lax.map(block_pairs, (to_blocks(middle_tile), to_blocks(nearby)))
    result = jnp.moveaxis(result, 0, 1)
    return result.reshape(result.shape[0], middle_tile.shape[1], middle_tile.shape[2], middle_tile.shape[3])

def advance(current, active_mask):
    positions = current[:3]
    payload_holder = jnp.concatenate([positions, active_mask], axis=0)
    local_density = jnp.zeros_like(active_mask)
    for displace_x, displace_y in stencil:
        local_density = local_density + grouped_by_block(pairwise_density, positions, adjacent_tiles(payload_holder, displace_x, displace_y), displace_x, displace_y)
    padded = local_density + (1.0 - active_mask)
    coefficient = stiffness * (local_density / rest_density - 1.0) / (padded * padded)
    inverse = 1.0 / padded
    middle_tile = jnp.concatenate([current, coefficient], axis=0)
    source = jnp.concatenate([current, active_mask, coefficient, inverse], axis=0)
    particle_acceleration = jnp.zeros_like(positions)
    for displace_x, displace_y in stencil:
        particle_acceleration = particle_acceleration + grouped_by_block(accel_pairs, middle_tile, adjacent_tiles(source, displace_x, displace_y), displace_x, displace_y)
    velocity = current[3:] + time_step * active_mask * particle_acceleration
    return jnp.concatenate([positions + time_step * velocity, velocity], axis=0)

def reference(positions, velocities, occupancy, cot_positions, cot_velocities):
    slot_ids = jnp.arange(P_SIZE, dtype=jnp.int32)
    active_mask = (slot_ids[None, None, :] < occupancy[:, :, None]).astype(jnp.float32)[None]
    stepper = jax.checkpoint(advance)

    def evolve(start_pos, start_vel):
        current = jnp.concatenate([start_pos, start_vel], axis=0)
        for step_id in range(STEPS):
            current = stepper(current, active_mask)
        return (current[:3], current[3:])
    outputs, pullback = jax.vjp(evolve, positions, velocities)
    grad_positions, grad_velocities = pullback((cot_positions, cot_velocities))
    return (grad_positions, grad_velocities)
```

```python
import functools

import jax
import jax.numpy as jnp
from jax import lax
from jax.experimental import pallas as pl
from jax.experimental.pallas import tpu as pltpu
from jax.sharding import PartitionSpec as P

STEPS = 4
DT = 0.05
MU = 0.15
MESH = pl.DeviceIdType.MESH
F32 = jnp.float32
I32 = jnp.int32
NJ, NI = 32, 8
SB = 32
NS = 128
REACH = 1.0001


def logical_to_mesh(gx, gy):
    pair = gx // 32
    s = gx + pair * (63 - 2 * gx)
    y = s // 8
    zz = s % 8
    z = zz + (y % 2) * (7 - 2 * zz)
    core = (gy * (3 - gy)) // 2
    x = pair * 3 + (gy // 2) * (1 - 2 * pair)
    return (y * 2 + x % 2) * 8 + z, (x // 2) * 2 + core


def mesh_to_logical(gx, gy):
    y = gx // 16
    xl = (gx // 8) % 2
    z = gx % 8
    pair = gy // 2
    core = gy % 2
    s = 8 * y + z + (y % 2) * (7 - 2 * z)
    return s + pair * (63 - 2 * s), core + (xl + pair * (1 - 2 * xl)) * (3 - 2 * core)


def halo_kernel(nx, ny, src, out, send_sem, recv_sem):
    gx, gy = mesh_to_logical(lax.axis_index("gx"), lax.axis_index("gy"))
    xm, xp = (gx + nx - 1) % nx, (gx + 1) % nx
    up, down = gy + 1 < ny, gy > 0
    barrier = pltpu.get_barrier_semaphore()

    def greet(x, y):
        pl.semaphore_signal(barrier, inc=1, device_id=logical_to_mesh(x, y), device_id_type=MESH)

    @pl.when(down)
    def _():
        for x in (xm, xp, gx):
            greet(x, gy - 1)

    @pl.when(up)
    def _():
        for x in (xm, xp, gx):
            greet(x, gy + 1)

    greet(xm, gy)
    greet(xp, gy)
    peers = 2 + 3 * (1 - gy // (ny - 1)) + 3 * ((gy + ny - 2) // (ny - 1))
    pl.semaphore_wait(barrier, peers)

    def go(k, start, dest, n, x, y, what):
        copy = pltpu.make_async_remote_copy(
            src_ref=src.at[:, pl.ds(start, n)],
            dst_ref=out.at[:, pl.ds(dest, n)],
            send_sem=send_sem.at[k],
            recv_sem=recv_sem.at[k],
            device_id=logical_to_mesh(x, y),
            device_id_type=MESH,
        )
        getattr(copy, what)()

    def along(what):
        go(0, 512, 0, 512, xp, gy, what)
        go(1, 0, 512, 512, xm, gy, what)

    def upward(what):
        go(4, 768, 2048, 256, xp, gy + 1, what)
        go(5, 256, 2304, 256, xm, gy + 1, what)
        go(2, 256, 1024, 256, gx, gy + 1, what)
        go(3, 768, 1280, 256, gx, gy + 1, what)

    def downward(what):
        go(8, 512, 2560, 256, xp, gy - 1, what)
        go(9, 0, 2816, 256, xm, gy - 1, what)
        go(6, 0, 1536, 256, gx, gy - 1, what)
        go(7, 512, 1792, 256, gx, gy - 1, what)

    @pl.when(up)
    def _():
        upward("start")

    @pl.when(down)
    def _():
        downward("start")

    along("start")
    along("wait")

    @pl.when(up)
    def _():
        upward("wait_send")
        downward("wait_recv")

    @pl.when(down)
    def _():
        downward("wait_send")
        upward("wait_recv")


VM = pl.BlockSpec(memory_space=pltpu.VMEM)
SM = pl.BlockSpec(memory_space=pltpu.SMEM)


def halo(own, nx, ny, cid):
    rows = own.shape[0]
    return pl.pallas_call(
        functools.partial(halo_kernel, nx, ny),
        out_shape=jax.ShapeDtypeStruct((rows, 3072), F32),
        in_specs=[VM],
        out_specs=VM,
        scratch_shapes=[pltpu.SemaphoreType.DMA((10,)), pltpu.SemaphoreType.DMA((10,))],
        compiler_params=pltpu.CompilerParams(
            collective_id=cid, has_side_effects=True, vmem_limit_bytes=2 << 20
        ),
        name=f"halo{rows}",
    )(own)


def iota(shape, dim):
    return lax.broadcasted_iota(I32, shape, dim)


def dot_t(a, b):
    return lax.dot_general(a, b, (((1,), (1,)), ((), ())), preferred_element_type=F32)


def plan_kernel(own, hal, ok, tab_j, tab_i, cnt, pre):
    sub = iota((NS, 128), 0)
    lane = iota((NS, 128), 1)
    upper = jnp.where(sub <= lane, 1.0, 0.0).astype(jnp.bfloat16)
    strict = jnp.where(lane < sub, 1.0, 0.0)

    def row(k):
        if k < NI:
            z = own[2:3, 128 * k : 128 * k + 128]
            live = own[6:7, 128 * k : 128 * k + 128] > 0.5
        else:
            s = 128 * (k - NI)
            good = ok[0:1, s : s + 128] > 0.5
            z = jnp.where(good, hal[2:3, s : s + 128], 0.0)
            live = jnp.where(good, hal[6:7, s : s + 128], 0.0) > 0.5
        bucket = jnp.clip((z * 8.0).astype(I32), 0, NS - 1)
        return jnp.where(live, bucket, -1)

    carry = jnp.zeros((NS, 1), F32)
    total_i = carry
    for k in range(NJ):
        hot = jnp.where(sub == row(k), 1.0, 0.0)
        count = jnp.dot(hot.astype(jnp.bfloat16), upper, preferred_element_type=F32)
        pre[:, 128 * k : 128 * k + 128] = count + carry - 1.0
        carry = carry + count[:, 127:128]
        if k == NI - 1:
            total_i = carry
    hi = lax.Precision.HIGHEST
    off_j = jnp.dot(strict, jnp.broadcast_to(carry, (NS, 128)), precision=hi, preferred_element_type=F32)
    off_i = jnp.dot(strict, jnp.broadcast_to(total_i, (NS, 128)), precision=hi, preferred_element_type=F32)

    def inverse(blocks, offset, nh, k, acc):
        b = row(k)
        rank = jnp.sum(
            jnp.where(sub == b, pre[:, 128 * k : 128 * k + 128] + offset, 0.0), axis=0, keepdims=True
        ).astype(I32)
        rank = jnp.where(b >= 0, rank, -128)
        high, low = rank >> 7, rank & 127
        eq = iota((nh, 128), 0) == high
        a = jnp.concatenate(
            [jnp.where(eq, iota((nh, 128), 1), 0), jnp.where(eq, k + 1, 0)], axis=0
        ).astype(F32).astype(jnp.bfloat16)
        hot = jnp.where(sub == low, 1.0, 0.0).astype(jnp.bfloat16)
        return acc + dot_t(a, hot), high, low

    acc = jnp.zeros((2 * NJ, 128), F32)
    for k in range(NJ):
        acc, _, _ = inverse(NJ, off_j, NJ, k, acc)
    tab_j[0:NJ, :] = acc[0:NJ].astype(I32)
    tab_j[NJ : 2 * NJ, :] = acc[NJ:].astype(I32) - 1
    acc = jnp.zeros((2 * NI, 128), F32)
    for k in range(NI):
        acc, high, low = inverse(NI, off_i, NI, k, acc)
        tab_i[16 + k : 17 + k, :] = high
        tab_i[24 + k : 25 + k, :] = jnp.maximum(low, 0)
    tab_i[0:NI, :] = acc[0:NI].astype(I32)
    tab_i[NI : 2 * NI, :] = acc[NI:].astype(I32) - 1
    nj = jnp.sum(carry, axis=0, keepdims=True)
    ni = jnp.sum(total_i, axis=0, keepdims=True)
    at = iota((1, 128), 1)
    blocks_j = (nj + 127.0).astype(I32) >> 7
    groups_i = (ni + (SB - 1.0)).astype(I32) >> 5
    cnt[...] = jnp.where(at == 0, blocks_j, groups_i)


def plan(own, hal, ok):
    return pl.pallas_call(
        plan_kernel,
        out_shape=(
            jax.ShapeDtypeStruct((2 * NJ, 128), I32),
            jax.ShapeDtypeStruct((32, 128), I32),
            jax.ShapeDtypeStruct((1, 128), I32),
        ),
        in_specs=[VM] * 3,
        out_specs=(VM, VM, VM),
        scratch_shapes=[pltpu.VMEM((NS, 4096), F32)],
        compiler_params=pltpu.CompilerParams(vmem_limit_bytes=8 << 20),
        name="plan",
    )(own, hal, ok)


def take(block, idx):
    return jnp.take_along_axis(block, idx, axis=1, mode="promise_in_bounds")


def gather(load, count, table, lane_row, blk_row):
    idx = jnp.broadcast_to(table[pl.ds(lane_row, 1), :], (8, 128))
    blk = jnp.broadcast_to(table[pl.ds(blk_row, 1), :], (8, 128))
    out = jnp.zeros((8, 128), F32)
    for k in range(count):
        out = jnp.where(blk == k, take(load(k), idx), out)
    return out


def source(own, hal, extra=None):
    def load(k):
        part = own[0:8, 128 * k : 128 * k + 128] if k < NI else hal[0:8, 128 * (k - NI) : 128 * (k - NI) + 128]
        if extra is not None:
            part = jnp.where(iota((8, 128), 0) < 6, part, 0.0) + extra[:, 128 * k : 128 * k + 128]
        return part

    return load


def block(ref, m):
    return ref[:, pl.ds(pl.multiple_of(m * 128, 128), 128)]


def put(ref, m, value):
    ref[:, pl.ds(pl.multiple_of(m * 128, 128), 128)] = value


def columns(ref, k, rows):
    ref[128 * k : 128 * k + 128, :] = rows.T


def columns_to_own(cols, rows, tab_i, store):
    for k in range(NI):
        rows[:, 128 * k : 128 * k + 128] = cols[128 * k : 128 * k + 128, :].T
    load = lambda m: rows[:, 128 * m : 128 * m + 128]
    for k in range(NI):
        store(k, gather(load, NI, tab_i, 24 + k, 16 + k))


def pairs(cnt, win, body, channels, cols, n_out):
    def group(g, _):
        at = pl.multiple_of(g * SB, SB)
        picked = [
            jnp.broadcast_to(ref[pl.ds(at, SB), c : c + 1], (SB, 128)) for ref, c in channels
        ]
        first = win[g >> 2, g & 3]
        last = win[g >> 2, (g & 3) + 4]
        sums = lax.fori_loop(
            first,
            last,
            lambda m, acc: body(m, picked, acc),
            tuple(jnp.zeros((SB, 128), F32) for _ in range(n_out)),
        )
        for c, total in enumerate(sums):
            cols[pl.ds(at, SB), c : c + 1] = jnp.sum(total, axis=1, keepdims=True)
        return 0

    lax.fori_loop(0, cnt[0, 1], group, 0)


def row_of(ref, c, m):
    return jnp.broadcast_to(ref[c : c + 1, pl.ds(pl.multiple_of(m * 128, 128), 128)], (SB, 128))


def geometry(mj, mr, m, xi, yi, zi, sx, sy):
    dx = row_of(mj, 0, m) - xi
    dy = row_of(mj, 1, m) - yi
    dz = row_of(mj, 2, m) - zi
    top = jnp.broadcast_to(mr[pl.ds(m, 1), :], (SB, 128)) - sx * row_of(mj, 6, m) - sy * row_of(mj, 7, m)
    q = jnp.maximum(top - (dx * dx + dy * dy + dz * dz), 0.0)
    return dx, dy, dz, q


GEO = (0, 1, 2, 6, 7)


def live_of(tab_i, k):
    return jnp.broadcast_to(tab_i[16 + k : 17 + k, :], (8, 128)) >= 0


def density_kernel(cnt, own, hal, attr_j, attr_i, tab_j, tab_i, mj, mr, ic, win, rho, cols, rows, zlo, zhi, win_s, sem):
    load = source(own, hal, attr_j)
    zlo[...] = jnp.full((NJ, 128), 1e30, F32)
    zhi[...] = jnp.full((NJ, 128), -1e30, F32)

    def fill(m, _):
        got = gather(load, NJ, tab_j, m, NJ + m)
        put(mj, m, got)
        held = tab_j[pl.ds(NJ + m, 1), :] >= 0
        mr[pl.ds(m, 1), :] = jnp.where(held, 1.0 - jnp.abs(got[6:7]) - jnp.abs(got[7:8]), -1.0)
        zlo[pl.ds(m, 1), :] = jnp.where(held, got[2:3], 1e30)
        zhi[pl.ds(m, 1), :] = jnp.where(held, got[2:3], -1e30)
        return 0

    lax.fori_loop(0, cnt[0, 0], fill, 0)
    load_i = source(own, hal, attr_i)
    z_rows = []
    for k in range(NI):
        got = gather(load_i, NI, tab_i, k, NI + k)
        columns(ic, k, got)
        z_rows.append(got[2:3])
    z_i = jnp.concatenate(z_rows, axis=0)
    held_i = tab_i[NI : 2 * NI, :] >= 0
    eye = iota((NJ, 128), 0) == iota((NJ, 128), 1)
    low_j = jnp.sum(jnp.where(eye, jnp.min(zlo[...], axis=1, keepdims=True), 0.0), axis=0, keepdims=True)
    high_j = jnp.sum(jnp.where(eye, jnp.max(zhi[...], axis=1, keepdims=True), 0.0), axis=0, keepdims=True)
    lane = iota((NI, 128), 1)
    windows = jnp.zeros((NI, 128), I32)
    lane_f = lane.astype(F32)
    for g in range(4):
        inside = held_i & (lane >= SB * g) & (lane < SB * g + SB)
        low = jnp.min(jnp.where(inside, z_i, 1e30), axis=1, keepdims=True)
        high = jnp.max(jnp.where(inside, z_i, -1e30), axis=1, keepdims=True)
        meets = (high_j > low - REACH) & (low_j < high + REACH) & (lane < NJ)
        first = jnp.min(jnp.where(meets, lane_f, 99.0), axis=1, keepdims=True).astype(I32)
        last = jnp.max(jnp.where(meets, lane_f + 1.0, 0.0), axis=1, keepdims=True).astype(I32)
        windows = jnp.where(lane == g, first, windows)
        windows = jnp.where(lane == g + 4, last, windows)
    win[...] = windows
    copy = pltpu.make_async_copy(win, win_s, sem)
    copy.start()
    copy.wait()

    def body(m, picked, acc):
        _, _, _, q = geometry(mj, mr, m, *picked)
        return (acc[0] + q * q * q,)

    pairs(cnt, win_s, body, [(ic, c) for c in GEO], cols, 1)

    def store(k, got):
        rho[:, 128 * k : 128 * k + 128] = MU * got

    columns_to_own(cols, rows, tab_i, store)


def call(kernel, name, ins, smem, outs, scratch=()):
    specs = [SM if i in smem else VM for i in range(len(ins))]
    return pl.pallas_call(
        kernel,
        out_shape=tuple(jax.ShapeDtypeStruct(s, t) for s, t in outs),
        in_specs=specs,
        out_specs=tuple(VM for _ in outs),
        scratch_shapes=list(scratch),
        compiler_params=pltpu.CompilerParams(vmem_limit_bytes=8 << 20),
        name=name,
    )(*ins)


COLS = ((1024, 8), F32)
OWN = ((8, 1024), F32)
WIDE = ((8, 4096), F32)


def density(cnt, own, hal, attr_j, attr_i, tab_j, tab_i):
    return call(
        density_kernel,
        "density",
        (cnt, own, hal, attr_j, attr_i, tab_j, tab_i),
        (0,),
        (WIDE, ((NJ, 128), F32), COLS, ((NI, 128), I32), OWN),
        (
            pltpu.VMEM((1024, 8), F32),
            pltpu.VMEM((8, 1024), F32),
            pltpu.VMEM((NJ, 128), F32),
            pltpu.VMEM((NJ, 128), F32),
            pltpu.SMEM((NI, 128), I32),
            pltpu.SemaphoreType.DMA,
        ),
    )


def pressure(rho_row, held):
    padded = jnp.where(held, rho_row, 1.0)
    inverse = 1.0 / padded
    return 24.0 * (padded - 1.0) * inverse * inverse, 3.0 * inverse


def pressure_tables(cnt, rho, rho_h, tab_j, tab_i, mc, cc):
    load = source(rho, rho_h)
    row8 = iota((8, 128), 0)

    def table(got, held):
        coef, inv = pressure(got[0:1], held)
        return jnp.where(row8 == 0, coef, jnp.where(row8 == 1, inv, 0.0))

    def fill(m, _):
        put(mc, m, table(gather(load, NJ, tab_j, m, NJ + m), tab_j[pl.ds(NJ + m, 1), :] >= 0))
        return 0

    lax.fori_loop(0, cnt[0, 0], fill, 0)
    for k in range(NI):
        columns(cc, k, table(gather(load, NI, tab_i, k, NI + k), tab_i[NI + k : NI + k + 1, :] >= 0))


def force_kernel(cnt, win, rho, rho_h, own, mj, mr, ic, tab_j, tab_i, mc, cc, new, cols, rows):
    pressure_tables(cnt, rho, rho_h, tab_j, tab_i, mc, cc)

    def body(m, picked, acc):
        xi, yi, zi, sx, sy, ux, uy, uz, ci = picked
        dx, dy, dz, q = geometry(mj, mr, m, xi, yi, zi, sx, sy)
        q2 = q * q
        push = (ci + row_of(mc, 0, m)) * q2
        drag = q2 * q * row_of(mc, 1, m) * (1.0 / 6.0)
        return (
            acc[0] + (drag * (row_of(mj, 3, m) - ux) - push * dx),
            acc[1] + (drag * (row_of(mj, 4, m) - uy) - push * dy),
            acc[2] + (drag * (row_of(mj, 5, m) - uz) - push * dz),
        )

    pairs(cnt, win, body, [(ic, c) for c in GEO + (3, 4, 5)] + [(cc, 0)], cols, 3)
    row8 = iota((8, 128), 0)

    def store(k, got):
        at = slice(128 * k, 128 * k + 128)
        v = [own[3 + c : 4 + c, at] + (DT * MU) * got[c : c + 1] for c in range(3)]
        x = [own[c : c + 1, at] + DT * v[c] for c in range(3)]
        new[0:3, at] = jnp.concatenate(x, axis=0)
        new[3:6, at] = jnp.concatenate(v, axis=0)
        new[6:8, at] = own[6:8, at]

    columns_to_own(cols, rows, tab_i, store)


def force(cnt, win, rho, rho_h, own, mj, mr, ic, tab_j, tab_i):
    return call(
        force_kernel,
        "force",
        (cnt, win, rho, rho_h, own, mj, mr, ic, tab_j, tab_i),
        (0, 1),
        (WIDE, COLS, OWN),
        (pltpu.VMEM((1024, 8), F32), pltpu.VMEM((8, 1024), F32)),
    )


def pressure_kernel(cnt, rho, rho_h, tab_j, tab_i, mc, cc):
    pressure_tables(cnt, rho, rho_h, tab_j, tab_i, mc, cc)


def pressure_only(cnt, rho, rho_h, tab_j, tab_i):
    return call(pressure_kernel, "pressure", (cnt, rho, rho_h, tab_j, tab_i), (0,), (WIDE, COLS))


def first_kernel(cnt, win, grad, grad_h, rho, mj, mr, ic, mc, tab_j, tab_i, mg, gc, out, cols, rows):
    load = source(grad, grad_h)

    def fill(m, _):
        put(mg, m, gather(load, NJ, tab_j, m, NJ + m))
        return 0

    lax.fori_loop(0, cnt[0, 0], fill, 0)
    for k in range(NI):
        columns(gc, k, gather(load, NI, tab_i, k, NI + k))

    def body(m, picked, acc):
        xi, yi, zi, sx, sy, ux, uy, uz, ax, ay, az = picked
        dx, dy, dz, q = geometry(mj, mr, m, xi, yi, zi, sx, sy)
        q2 = q * q
        q3 = q2 * q
        bx, by, bz = row_of(mg, 0, m), row_of(mg, 1, m), row_of(mg, 2, m)
        dh = dx * (ax - bx) + dy * (ay - by) + dz * (az - bz)
        ub = (row_of(mj, 3, m) - ux) * bx + (row_of(mj, 4, m) - uy) * by + (row_of(mj, 5, m) - uz) * bz
        return (
            acc[0] + q2 * dh,
            acc[1] + q3 * ub,
            acc[2] + q3 * row_of(mc, 1, m),
            acc[3] + q3 * bx,
            acc[4] + q3 * by,
            acc[5] + q3 * bz,
        )

    pairs(cnt, win, body, [(ic, c) for c in GEO + (3, 4, 5)] + [(gc, 0), (gc, 1), (gc, 2)], cols, 6)

    def store(k, got):
        at = slice(128 * k, 128 * k + 128)
        held = live_of(tab_i, k)[0:1]
        p = jnp.where(held, rho[0:1, at], 1.0)
        inv = 1.0 / p
        inv2 = inv * inv
        by_coef = (-6.0 * MU) * got[0:1]
        by_pad = (0.5 * MU) * inv2 * got[1:2]
        g_rho = by_coef * (4.0 * inv2 - 8.0 * (p - 1.0) * inv2 * inv) + by_pad
        out[0:1, at] = jnp.where(held, 6.0 * g_rho, 0.0)
        out[1:4, at] = (-0.5 * MU) * (grad[0:3, at] * (got[2:3] * (1.0 / 3.0)) - inv * got[3:6])
        out[4:8, at] = jnp.zeros((4, 128), F32)

    columns_to_own(cols, rows, tab_i, store)


def first_sweep(*ins):
    return call(
        first_kernel,
        "adjoint1",
        ins,
        (0, 1),
        (WIDE, COLS, OWN),
        (pltpu.VMEM((1024, 8), F32), pltpu.VMEM((8, 1024), F32)),
    )


def second_kernel(final, cnt, win, part, part_h, carry, mj, mr, ic, mc, cc, mg, gc, tab_j, tab_i, grad, new, mp, pc, cols, rows):
    load = source(part, part_h)

    def fill(m, _):
        put(mp, m, gather(load, NJ, tab_j, m, NJ + m))
        return 0

    lax.fori_loop(0, cnt[0, 0], fill, 0)
    for k in range(NI):
        columns(pc, k, gather(load, NI, tab_i, k, NI + k))

    def body(m, picked, acc):
        xi, yi, zi, sx, sy, ux, uy, uz, ax, ay, az, ci, pi, ri = picked
        dx, dy, dz, q = geometry(mj, mr, m, xi, yi, zi, sx, sy)
        bx, by, bz = row_of(mg, 0, m), row_of(mg, 1, m), row_of(mg, 2, m)
        hx, hy, hz = ax - bx, ay - by, az - bz
        wx, wy, wz = row_of(mj, 3, m) - ux, row_of(mj, 4, m) - uy, row_of(mj, 5, m) - uz
        dh = dx * hx + dy * hy + dz * hz
        ua = wx * ax + wy * ay + wz * az
        ub = wx * bx + wy * by + wz * bz
        coef = ci + row_of(mc, 0, m)
        along = q * (q * (ua * row_of(mc, 1, m) - ub * pi + (ri + row_of(mp, 0, m))) - 4.0 * coef * dh)
        across = coef * (q * q)
        return (
            acc[0] + (along * dx + across * hx),
            acc[1] + (along * dy + across * hy),
            acc[2] + (along * dz + across * hz),
        )

    channels = [(ic, c) for c in GEO + (3, 4, 5)] + [(gc, 0), (gc, 1), (gc, 2), (cc, 0), (cc, 1), (pc, 0)]
    pairs(cnt, win, body, channels, cols, 3)

    def store(k, got):
        at = slice(128 * k, 128 * k + 128)
        gp = carry[0:3, at] + MU * got[0:3]
        gv = carry[3:6, at] + part[1:4, at]
        if not final:
            gv = gv + DT * gp
            held = live_of(tab_i, k)[0:3]
            grad[0:3, at] = jnp.where(held, DT * gv, 0.0)
            grad[3:8, at] = jnp.zeros((5, 128), F32)
        else:
            grad[:, at] = jnp.zeros((8, 128), F32)
        new[0:3, at] = gp
        new[3:6, at] = gv
        new[6:8, at] = jnp.zeros((2, 128), F32)

    columns_to_own(cols, rows, tab_i, store)


def second_sweep(final, *ins):
    return call(
        functools.partial(second_kernel, final),
        "adjoint2",
        ins,
        (0, 1),
        (OWN, OWN),
        (
            pltpu.VMEM((8, 4096), F32),
            pltpu.VMEM((1024, 8), F32),
            pltpu.VMEM((1024, 8), F32),
            pltpu.VMEM((8, 1024), F32),
        ),
    )


def tile_offsets():
    own = [(0, 0), (0, 1), (1, 0), (1, 1)]
    sides = [(-1, 0), (-1, 1), (2, 0), (2, 1), (0, -1), (1, -1), (0, 2), (1, 2)]
    corners = [(-1, -1), (2, -1), (-1, 2), (2, 2)]
    return own + sides + corners


def attributes():
    def edge(a):
        return {2: -0.5, -1: 0.5}.get(a, 0.0)

    wide = [[float(a), float(b), 0.0, 0.0, 0.0, 0.0, edge(a), edge(b)] for a, b in tile_offsets()]
    near = [[float(a), float(b), 0.0, 0.0, 0.0, 0.0, 2.0 * a - 1, 2.0 * b - 1] for a, b in tile_offsets()[:4]]
    attr_j = jnp.repeat(jnp.array(wide, F32).T, 256, axis=1)
    attr_i = jnp.repeat(jnp.array(near, F32).T, 256, axis=1)
    return attr_j, attr_i


def per_device(nx, ny, positions, velocities, occupancy, cot_positions, cot_velocities):
    flat = lambda a: a.reshape(3, 1024)
    slots = lax.broadcasted_iota(I32, (2, 2, 256), 2)
    live = (slots < occupancy[:, :, None]).astype(F32).reshape(1, 1024)
    zero = jnp.zeros((1, 1024), F32)
    state = jnp.concatenate(
        [flat(positions), flat(velocities), live, zero, flat(cot_positions), flat(cot_velocities), zero, zero], axis=0
    )
    there = [(a * ny + b, logical_to_mesh(a, b)) for a in range(nx) for b in range(ny)]
    there = [(s, d[0] * ny + d[1]) for s, d in there]
    state = lax.ppermute(state, ("gx", "gy"), there)
    _, gy = mesh_to_logical(lax.axis_index("gx"), lax.axis_index("gy"))
    lane = lax.broadcasted_iota(I32, (1, 3072), 1)
    lower = ((lane >= 1024) & (lane < 1536)) | ((lane >= 2048) & (lane < 2560))
    upper = ((lane >= 1536) & (lane < 2048)) | (lane >= 2560)
    ok = jnp.where((lower & (gy == 0)) | (upper & (gy == ny - 1)), 0.0, 1.0)
    grad_vel = state[11:14] + DT * state[8:11]
    grad = DT * state[6:7] * grad_vel
    pad2 = jnp.zeros((2, 1024), F32)
    carry = jnp.concatenate([state[8:11], grad_vel, pad2], axis=0)
    own = state[0:8]
    start = jnp.concatenate([own, grad, jnp.zeros((5, 1024), F32)], axis=0)
    attr_j, attr_i = attributes()

    hal16 = halo(start, nx, ny, 1)
    hal = hal16[0:8]
    grad, grad_h = start[8:16], hal16[8:16]
    tab_j, tab_i, cnt = plan(own, hal, ok)
    history = []
    for step in range(STEPS):
        if step:
            hal = halo(own, nx, ny, 0)
        mj, mr, ic, win, rho = density(cnt, own, hal, attr_j, attr_i, tab_j, tab_i)
        rho_h = halo(rho, nx, ny, 0)
        if step + 1 < STEPS:
            mc, cc, own = force(cnt, win, rho, rho_h, own, mj, mr, ic, tab_j, tab_i)
        else:
            mc, cc = pressure_only(cnt, rho, rho_h, tab_j, tab_i)
        history.append((win, rho, mj, mr, ic, mc, cc))
    for step in reversed(range(STEPS)):
        win, rho, mj, mr, ic, mc, cc = history[step]
        mg, gc, part = first_sweep(cnt, win, grad, grad_h, rho, mj, mr, ic, mc, tab_j, tab_i)
        part_h = halo(part, nx, ny, 0)
        grad, carry = second_sweep(step == 0, cnt, win, part, part_h, carry, mj, mr, ic, mc, cc, mg, gc, tab_j, tab_i)
        if step:
            grad_h = halo(grad, nx, ny, 0)
    back = [(d, s) for s, d in there]
    result = lax.ppermute(carry, ("gx", "gy"), back)
    return result[0:3].reshape(positions.shape), result[3:6].reshape(positions.shape)


def solution(mesh):
    spec = P(None, "gx", "gy", None)
    return jax.shard_map(
        functools.partial(per_device, mesh.shape["gx"], mesh.shape["gy"]),
        mesh=mesh,
        in_specs=(spec, spec, P("gx", "gy"), spec, spec),
        out_specs=(spec, spec),
        check_vma=False,
    )
```

```python
import functools

import jax
import jax.numpy as jnp
from jax import lax
from jax.experimental import pallas as pl
from jax.experimental.pallas import tpu as pltpu
from jax.sharding import PartitionSpec as P

STEPS = 4
DT = 0.05
MU = 0.15
MESH = pl.DeviceIdType.MESH
F32 = jnp.float32
I32 = jnp.int32
NJ, NI = 32, 8
NK = 30
SB = 32
NS = 128
REACH = 1.0001


def logical_to_mesh(column, half):
    y = column // 32
    s = column % 32
    s = s + (y % 2) * (31 - 2 * s)
    z = s // 4
    x = s % 4
    x = x + (z % 2) * (3 - 2 * x)
    return (y * 2 + x % 2) * 8 + z, (x // 2) * 2 + half


def mesh_to_logical(gx, gy):
    y = gx // 16
    z = gx % 8
    x = (gy // 2) * 2 + (gx // 8) % 2
    s = 4 * z + x + (z % 2) * (3 - 2 * x)
    return 32 * y + s + (y % 2) * (31 - 2 * s), gy % 2


def halo_kernel(ring, src, out, send_sem, recv_sem):
    column, half = mesh_to_logical(lax.axis_index("gx"), lax.axis_index("gy"))
    left, right, other = (column + ring - 1) % ring, (column + 1) % ring, 1 - half
    barrier = pltpu.get_barrier_semaphore()
    for who in ((left, half), (right, half), (left, other), (right, other), (column, other)):
        pl.semaphore_signal(barrier, inc=1, device_id=logical_to_mesh(*who), device_id_type=MESH)
    pl.semaphore_wait(barrier, 5)
    rim = pl.multiple_of(768 * other, 128)

    def copy(k, start, dest, n, who):
        return pltpu.make_async_remote_copy(
            src_ref=src.at[:, pl.ds(start, n)],
            dst_ref=out.at[:, pl.ds(dest, n)],
            send_sem=send_sem.at[k],
            recv_sem=recv_sem.at[k],
            device_id=logical_to_mesh(*who),
            device_id_type=MESH,
        )

    copies = [
        copy(0, rim, 2304, 256, (right, other)),
        copy(1, rim, 2560, 256, (left, other)),
        copy(2, 0, 0, 1024, (right, half)),
        copy(3, 0, 1024, 1024, (left, half)),
        copy(4, rim, 2048, 256, (column, other)),
    ]
    for c in copies:
        c.start()
    for c in copies:
        c.wait()


VM = pl.BlockSpec(memory_space=pltpu.VMEM)
SM = pl.BlockSpec(memory_space=pltpu.SMEM)


def halo(own, ring, cid):
    rows = own.shape[0]
    return pl.pallas_call(
        functools.partial(halo_kernel, ring),
        out_shape=jax.ShapeDtypeStruct((rows, 3072), F32),
        in_specs=[VM],
        out_specs=VM,
        scratch_shapes=[pltpu.SemaphoreType.DMA((5,)), pltpu.SemaphoreType.DMA((5,))],
        compiler_params=pltpu.CompilerParams(
            collective_id=cid, has_side_effects=True, vmem_limit_bytes=2 << 20
        ),
        name=f"halo{rows}",
    )(own)


def iota(shape, dim):
    return lax.broadcasted_iota(I32, shape, dim)


def dot_t(a, b):
    return lax.dot_general(a, b, (((1,), (1,)), ((), ())), preferred_element_type=F32)


def plan_kernel(own, hal, tab_j, tab_i, cnt, pre):
    sub = iota((NS, 128), 0)
    lane = iota((NS, 128), 1)
    upper = jnp.where(sub <= lane, 1.0, 0.0).astype(jnp.bfloat16)
    strict = jnp.where(lane < sub, 1.0, 0.0)

    def row(k):
        if k < NI:
            z = own[2:3, 128 * k : 128 * k + 128]
            live = own[6:7, 128 * k : 128 * k + 128] > 0.5
        else:
            s = 128 * (k - NI)
            z = hal[2:3, s : s + 128]
            live = hal[6:7, s : s + 128] > 0.5
        bucket = jnp.clip((z * 8.0).astype(I32), 0, NS - 1)
        return jnp.where(live, bucket, -1)

    carry = jnp.zeros((NS, 1), F32)
    total_i = carry
    for k in range(NK):
        hot = jnp.where(sub == row(k), 1.0, 0.0)
        count = jnp.dot(hot.astype(jnp.bfloat16), upper, preferred_element_type=F32)
        pre[:, 128 * k : 128 * k + 128] = count + carry - 1.0
        carry = carry + count[:, 127:128]
        if k == NI - 1:
            total_i = carry
    hi = lax.Precision.HIGHEST
    off_j = jnp.dot(strict, jnp.broadcast_to(carry, (NS, 128)), precision=hi, preferred_element_type=F32)
    off_i = jnp.dot(strict, jnp.broadcast_to(total_i, (NS, 128)), precision=hi, preferred_element_type=F32)

    def inverse(blocks, offset, nh, k, acc):
        b = row(k)
        rank = jnp.sum(
            jnp.where(sub == b, pre[:, 128 * k : 128 * k + 128] + offset, 0.0), axis=0, keepdims=True
        ).astype(I32)
        rank = jnp.where(b >= 0, rank, -128)
        high, low = rank >> 7, rank & 127
        eq = iota((nh, 128), 0) == high
        a = jnp.concatenate(
            [jnp.where(eq, iota((nh, 128), 1), 0), jnp.where(eq, k + 1, 0)], axis=0
        ).astype(F32).astype(jnp.bfloat16)
        hot = jnp.where(sub == low, 1.0, 0.0).astype(jnp.bfloat16)
        return acc + dot_t(a, hot), high, low

    acc = jnp.zeros((2 * NJ, 128), F32)
    for k in range(NK):
        acc, _, _ = inverse(NJ, off_j, NJ, k, acc)
    tab_j[0:NJ, :] = acc[0:NJ].astype(I32)
    tab_j[NJ : 2 * NJ, :] = acc[NJ:].astype(I32) - 1
    acc = jnp.zeros((2 * NI, 128), F32)
    for k in range(NI):
        acc, high, low = inverse(NI, off_i, NI, k, acc)
        tab_i[16 + k : 17 + k, :] = high
        tab_i[24 + k : 25 + k, :] = jnp.maximum(low, 0)
    tab_i[0:NI, :] = acc[0:NI].astype(I32)
    tab_i[NI : 2 * NI, :] = acc[NI:].astype(I32) - 1
    nj = jnp.sum(carry, axis=0, keepdims=True)
    ni = jnp.sum(total_i, axis=0, keepdims=True)
    at = iota((1, 128), 1)
    blocks_j = (nj + 127.0).astype(I32) >> 7
    groups_i = (ni + (SB - 1.0)).astype(I32) >> 5
    cnt[...] = jnp.where(at == 0, blocks_j, groups_i)


def plan(own, hal):
    return pl.pallas_call(
        plan_kernel,
        out_shape=(
            jax.ShapeDtypeStruct((2 * NJ, 128), I32),
            jax.ShapeDtypeStruct((32, 128), I32),
            jax.ShapeDtypeStruct((1, 128), I32),
        ),
        in_specs=[VM] * 2,
        out_specs=(VM, VM, VM),
        scratch_shapes=[pltpu.VMEM((NS, 4096), F32)],
        compiler_params=pltpu.CompilerParams(vmem_limit_bytes=8 << 20),
        name="plan",
    )(own, hal)


def take(block, idx):
    return jnp.take_along_axis(block, idx, axis=1, mode="promise_in_bounds")


def gather(load, count, table, lane_row, blk_row):
    idx = jnp.broadcast_to(table[pl.ds(lane_row, 1), :], (8, 128))
    blk = jnp.broadcast_to(table[pl.ds(blk_row, 1), :], (8, 128))
    out = jnp.zeros((8, 128), F32)
    for k in range(count):
        out = jnp.where(blk == k, take(load(k), idx), out)
    return out


def spread(own, hal, stage, n):
    for k in range(NK):
        part = own[:, 128 * k : 128 * k + 128] if k < NI else hal[:, 128 * (k - NI) : 128 * (k - NI) + 128]
        for c in range(n):
            stage[NJ * c + k : NJ * c + k + 1, :] = part[c : c + 1]


def pick(stage, c, groups, idx, blk):
    sub = iota((8, 128), 0)
    out = jnp.zeros((8, 128), F32)
    for j in range(groups):
        part = stage[NJ * c + 8 * j : NJ * c + 8 * j + 8, :]
        out = jnp.where(blk == sub + 8 * j, take(part, idx), out)
    return jnp.sum(out, axis=0, keepdims=True)


def entry(table, lane_row, blk_row):
    idx = jnp.broadcast_to(table[pl.ds(lane_row, 1), :], (8, 128))
    return idx, jnp.broadcast_to(table[pl.ds(blk_row, 1), :], (8, 128))


def each_block(cnt, fill, together=8):
    def several(b, _):
        for n in range(together):
            fill(together * b + n, 0)
        return 0

    lax.fori_loop(0, (cnt[0, 0] + together - 1) // together, several, 0)


def block(ref, m):
    return ref[:, pl.ds(pl.multiple_of(m * 128, 128), 128)]


def put(ref, m, value):
    ref[:, pl.ds(pl.multiple_of(m * 128, 128), 128)] = value


def columns(ref, k, rows):
    ref[128 * k : 128 * k + 128, :] = rows.T


def sums_to_own(cnt, sums, n_out, cols, rows, tab_i, store):
    def reduce(b, _):
        for n in range(4):
            at = pl.multiple_of(b * 512 + 128 * n, 128)
            for c in range(n_out):
                cols[pl.ds(at, 128), c : c + 1] = jnp.sum(sums[c, pl.ds(at, 128), :], axis=1, keepdims=True)
        for n in range(4):
            at = pl.multiple_of(b * 512 + 128 * n, 128)
            rows[:, pl.ds(at, 128)] = cols[pl.ds(at, 128), :].T
        return 0

    lax.fori_loop(0, (cnt[0, 1] + 15) >> 4, reduce, 0)
    load = lambda m: rows[:, 128 * m : 128 * m + 128]
    for k in range(NI):
        store(k, gather(load, NI, tab_i, 24 + k, 16 + k))


def broadcast_columns(cnt, channels, sums, n_out):
    def one(b, _):
        at = pl.multiple_of(b * 128, 128)
        for ref, c, wide, n in channels:
            wide[n, pl.ds(at, 128), :] = jnp.broadcast_to(ref[pl.ds(at, 128), c : c + 1], (128, 128))
        for c in range(n_out):
            sums[c, pl.ds(at, 128), :] = jnp.zeros((128, 128), F32)
        return 0

    lax.fori_loop(0, (cnt[0, 1] + 3) >> 2, one, 0)


def pairs(cnt, win, rows, body, mine, sums):
    def each(m, _):
        picked = rows(m)
        first = win[m, 0]

        def chunk(n, _):
            at = pl.multiple_of((first + 4 * n) * 8, 8)
            terms = body(picked, *[wide[c, pl.ds(at, SB), :] for wide, c in mine])
            for c, term in enumerate(terms):
                sums[c, pl.ds(at, SB), :] += term
            return 0

        lax.fori_loop(0, win[m, 1], chunk, 0)
        return 0

    lax.fori_loop(0, cnt[0, 0], each, 0)


def places(*refs):
    return [(ref, c) for ref, count in refs for c in range(count)]


def row_of(ref, c, m):
    return ref[c : c + 1, pl.ds(pl.multiple_of(m * 128, 128), 128)]


def spot(mj, m):
    return [row_of(mj, c, m) for c in GEO]


def geometry(spots, xi, yi, zi, bi):
    xj, yj, zj, bj = [jnp.broadcast_to(r, (SB, 128)) for r in spots]
    dx, dy, dz, db = xj - xi, yj - yi, zj - zi, bj - bi
    top = jnp.minimum(2.0 - db * db, 1.0)
    q = jnp.maximum(top - (dx * dx + dy * dy + dz * dz), 0.0)
    return dx, dy, dz, q


GEO = (0, 1, 2, 6)


def live_of(tab_i, k):
    return jnp.broadcast_to(tab_i[16 + k : 17 + k, :], (8, 128)) >= 0


def density_kernel(cnt, own, hal, attr_j, attr_i, tab_j, tab_i, mj, ic, win, rho, geo, cols, rows, zlo, zhi, win_s, sem, stage, sums):
    body6 = iota((8, 128), 0) < 6
    for k in range(NK):
        part = own[0:8, 128 * k : 128 * k + 128] if k < NI else hal[0:8, 128 * (k - NI) : 128 * (k - NI) + 128]
        stage[:, 128 * k : 128 * k + 128] = jnp.where(body6, part, 0.0) + attr_j[:, 128 * k : 128 * k + 128]
    load = lambda k: stage[:, 128 * k : 128 * k + 128]
    zlo[...] = jnp.full((NJ, 128), 1e30, F32)
    zhi[...] = jnp.full((NJ, 128), -1e30, F32)

    def fill(m, _):
        got = gather(load, NK, tab_j, m, NJ + m)
        held = tab_j[pl.ds(NJ + m, 1), :] >= 0
        put(mj, m, jnp.where((iota((8, 128), 0) == 6) & ~held, 1000.0, got))
        zlo[pl.ds(m, 1), :] = jnp.where(held, got[2:3], 1e30)
        zhi[pl.ds(m, 1), :] = jnp.where(held, got[2:3], -1e30)
        return 0

    each_block(cnt, fill, 4)
    body6 = iota((8, 128), 0) < 6

    def load_i(k):
        at = slice(128 * k, 128 * k + 128)
        return jnp.where(body6, own[:, at], 0.0) + attr_i[:, at]

    z_rows = []
    for k in range(NI):
        got = gather(load_i, NI, tab_i, k, NI + k)
        columns(ic, k, got)
        z_rows.append(got[2:3])
    low = jnp.min(zlo[...], axis=1, keepdims=True) - REACH
    high = jnp.max(zhi[...], axis=1, keepdims=True) + REACH
    first = jnp.full((NJ, 128), 4096, I32)
    last = jnp.zeros((NJ, 128), I32)
    for k in range(NI):
        held = tab_i[NI + k : NI + k + 1, :] >= 0
        meets = (z_rows[k] > low) & (z_rows[k] < high) & held
        at = iota((NJ, 128), 1) + 128 * k
        first = jnp.minimum(first, jnp.where(meets, at, 4096))
        last = jnp.maximum(last, jnp.where(meets, at + 1, 0))
    first = jnp.min(first.astype(F32), axis=1, keepdims=True).astype(I32) >> 3
    last = jnp.max(last.astype(F32), axis=1, keepdims=True).astype(I32)
    chunks = jnp.maximum(last - 8 * first + (SB - 1), 0) >> 5
    windows = jnp.where(iota((NJ, 128), 1) == 0, first, chunks)
    win[...] = windows
    copy = pltpu.make_async_copy(win, win_s, sem)
    copy.start()
    broadcast_columns(cnt, [(ic, c, geo, n) for n, c in enumerate(GEO)], sums, 1)
    copy.wait()

    def body(spots, *mine):
        _, _, _, q = geometry(spots, *mine)
        return (q * q * q,)

    pairs(cnt, win_s, lambda m: spot(mj, m), body, places((geo, 4)), sums)

    def store(k, got):
        rho[:, 128 * k : 128 * k + 128] = MU * got[0:1]

    sums_to_own(cnt, sums, 1, cols, rows, tab_i, store)


def call(kernel, name, ins, smem, outs, scratch=()):
    specs = [SM if i in smem else VM for i in range(len(ins))]
    return pl.pallas_call(
        kernel,
        out_shape=tuple(jax.ShapeDtypeStruct(s, t) for s, t in outs),
        in_specs=specs,
        out_specs=tuple(VM for _ in outs),
        scratch_shapes=list(scratch),
        compiler_params=pltpu.CompilerParams(vmem_limit_bytes=12 << 20),
        name=name,
    )(*ins)


def scratch(n_in, n_out):
    return (
        pltpu.VMEM((1024, 8), F32),
        pltpu.VMEM((8, 1024), F32),
        pltpu.VMEM((8 * NJ, 128), F32),
        pltpu.VMEM((n_in, 1024 + SB, 128), F32),
        pltpu.VMEM((n_out, 1024 + SB, 128), F32),
    )


COLS = ((1024, 8), F32)
OWN = ((8, 1024), F32)
ROW = ((1, 1024), F32)


def lanes(n):
    return ((n, 1024 + SB, 128), F32)


GRAD = ((4, 1024), F32)
WIDE = ((8, 4096), F32)


def density(cnt, own, hal, attr_j, attr_i, tab_j, tab_i):
    return call(
        density_kernel,
        "density",
        (cnt, own, hal, attr_j, attr_i, tab_j, tab_i),
        (0,),
        (WIDE, COLS, ((NJ, 128), I32), ROW, lanes(4)),
        (
            pltpu.VMEM((1024, 8), F32),
            pltpu.VMEM((8, 1024), F32),
            pltpu.VMEM((NJ, 128), F32),
            pltpu.VMEM((NJ, 128), F32),
            pltpu.SMEM((NJ, 128), I32),
            pltpu.SemaphoreType.DMA,
            pltpu.VMEM((8, 4096), F32),
            pltpu.VMEM((1, 1024 + SB, 128), F32),
        ),
    )


def pressure(rho_row, held):
    padded = jnp.where(held, rho_row, 1.0)
    inverse = 1.0 / padded
    return 24.0 * (padded - 1.0) * inverse * inverse, 3.0 * inverse


def pressure_tables(cnt, rho, rho_h, tab_j, tab_i, mc, cc, stage):
    spread(rho, rho_h, stage, 1)
    row8 = iota((8, 128), 0)

    def table(got, held):
        coef, inv = pressure(got, held)
        return jnp.where(row8 == 0, coef, jnp.where(row8 == 1, inv, 0.0))

    def fill(m, _):
        idx, blk = entry(tab_j, m, NJ + m)
        put(mc, m, table(pick(stage, 0, 4, idx, blk), tab_j[pl.ds(NJ + m, 1), :] >= 0))
        return 0

    each_block(cnt, fill)
    for k in range(NI):
        idx, blk = entry(tab_i, k, NI + k)
        columns(cc, k, table(pick(stage, 0, 1, idx, blk), tab_i[NI + k : NI + k + 1, :] >= 0))


def force_kernel(cnt, win, rho, rho_h, own, mj, geo, tab_j, tab_i, mc, cc, new, cols, rows, stage, wide, sums):
    pressure_tables(cnt, rho, rho_h, tab_j, tab_i, mc, cc, stage)
    broadcast_columns(cnt, [(cc, 0, wide, 0)], sums, 4)

    def rows_at(m):
        return spot(mj, m), [row_of(mj, c, m) for c in (3, 4, 5)], row_of(mc, 0, m), row_of(mc, 1, m) * (1.0 / 6.0)

    def body(other, xi, yi, zi, bi, ci):
        spots, (vx, vy, vz), cj, pj = other
        dx, dy, dz, q = geometry(spots, xi, yi, zi, bi)
        q2 = q * q
        push = (ci + cj) * q2
        drag = q2 * q * pj
        return drag * vx - push * dx, drag * vy - push * dy, drag * vz - push * dz, drag

    pairs(cnt, win, rows_at, body, places((geo, 4), (wide, 1)), sums)


    def store(k, got):
        at = slice(128 * k, 128 * k + 128)
        v = [own[3 + c : 4 + c, at] for c in range(3)]
        v = [v[c] + (DT * MU) * (got[c : c + 1] - v[c] * got[3:4]) for c in range(3)]
        x = [own[c : c + 1, at] + DT * v[c] for c in range(3)]
        new[0:3, at] = jnp.concatenate(x, axis=0)
        new[3:6, at] = jnp.concatenate(v, axis=0)
        new[6:8, at] = own[6:8, at]

    sums_to_own(cnt, sums, 4, cols, rows, tab_i, store)


def force(cnt, win, rho, rho_h, own, mj, geo, tab_j, tab_i):
    return call(
        force_kernel,
        "force",
        (cnt, win, rho, rho_h, own, mj, geo, tab_j, tab_i),
        (0, 1),
        (WIDE, COLS, OWN),
        scratch(1, 4),
    )


def pressure_kernel(cnt, rho, rho_h, tab_j, tab_i, mc, cc, stage):
    pressure_tables(cnt, rho, rho_h, tab_j, tab_i, mc, cc, stage)


def pressure_only(cnt, rho, rho_h, tab_j, tab_i):
    return call(pressure_kernel, "pressure", (cnt, rho, rho_h, tab_j, tab_i), (0,), (WIDE, COLS), scratch(0, 0)[2:3])


def first_kernel(cnt, win, own, grad, grad_h, rho, mj, geo, mc, tab_j, tab_i, mg, ga, out, by_vel, gc, cols, rows, stage, wide, sums):
    spread(grad, grad_h, stage, 3)
    none = jnp.zeros((5, 128), F32)

    def fill(m, _):
        idx, blk = entry(tab_j, m, NJ + m)
        got = [pick(stage, c, 4, idx, blk) for c in range(3)]
        put(mg, m, jnp.concatenate(got + [none], axis=0))
        return 0

    each_block(cnt, fill)
    for k in range(NI):
        idx, blk = entry(tab_i, k, NI + k)
        got = [pick(stage, c, 1, idx, blk) for c in range(3)]
        columns(gc, k, jnp.concatenate(got + [none], axis=0))
    broadcast_columns(cnt, [(gc, c, ga, c) for c in range(3)], sums, 6)

    def rows_at(m):
        g = [row_of(mg, c, m) for c in range(3)]
        v = [row_of(mj, c, m) for c in (3, 4, 5)]
        return spot(mj, m), g, v[0] * g[0] + v[1] * g[1] + v[2] * g[2], row_of(mc, 1, m)

    def body(other, xi, yi, zi, bi, ax, ay, az):
        spots, (bx, by, bz), work, pj = other
        dx, dy, dz, q = geometry(spots, xi, yi, zi, bi)
        q2 = q * q
        q3 = q2 * q
        dh = dx * (ax - bx) + dy * (ay - by) + dz * (az - bz)
        return q2 * dh, q3 * work, q3 * pj, q3 * bx, q3 * by, q3 * bz

    pairs(cnt, win, rows_at, body, places((geo, 4), (ga, 3)), sums)

    def store(k, got):
        at = slice(128 * k, 128 * k + 128)
        held = live_of(tab_i, k)[0:1]
        p = jnp.where(held, rho[0:1, at], 1.0)
        inv = 1.0 / p
        inv2 = inv * inv
        by_coef = (-6.0 * MU) * got[0:1]
        drag = got[1:2] - (own[3:4, at] * got[3:4] + own[4:5, at] * got[4:5] + own[5:6, at] * got[5:6])
        by_pad = (0.5 * MU) * inv2 * drag
        g_rho = by_coef * (4.0 * inv2 - 8.0 * (p - 1.0) * inv2 * inv) + by_pad
        out[0:1, at] = jnp.where(held, 6.0 * g_rho, 0.0)
        by_vel[0:3, at] = (-0.5 * MU) * (grad[0:3, at] * (got[2:3] * (1.0 / 3.0)) - inv * got[3:6])
        by_vel[3:4, at] = jnp.zeros((1, 128), F32)

    sums_to_own(cnt, sums, 6, cols, rows, tab_i, store)


def first_sweep(*ins):
    return call(
        first_kernel,
        "adjoint1",
        ins,
        (0, 1),
        (WIDE, lanes(3), ROW, GRAD),
        (pltpu.VMEM((1024, 8), F32),) + scratch(1, 6),
    )


def second_kernel(final, cnt, win, part, part_h, by_vel, carry, mj, ic, geo, mc, cc, mg, ga, tab_j, tab_i, grad, new, mp, pc, cols, rows, stage, wide, sums):
    spread(part, part_h, stage, 1)

    def fill(m, _):
        idx, blk = entry(tab_j, m, NJ + m)
        put(mp, m, jnp.broadcast_to(pick(stage, 0, 4, idx, blk), (8, 128)))
        return 0

    each_block(cnt, fill)
    for k in range(NI):
        idx, blk = entry(tab_i, k, NI + k)
        columns(pc, k, jnp.broadcast_to(pick(stage, 0, 1, idx, blk), (8, 128)))
    taken = [(ic, 3), (ic, 4), (ic, 5), (cc, 0), (cc, 1), (pc, 0)]
    broadcast_columns(cnt, [(ref, c, wide, n) for n, (ref, c) in enumerate(taken)], sums, 3)

    def rows_at(m):
        v = [row_of(mj, c, m) for c in (3, 4, 5)]
        g = [row_of(mg, c, m) for c in range(3)]
        return spot(mj, m), v, g, row_of(mc, 0, m), row_of(mc, 1, m), row_of(mp, 0, m)

    def body(other, xi, yi, zi, bi, ax, ay, az, ux, uy, uz, ci, pi, ri):
        spots, (vx, vy, vz), (bx, by, bz), cj, pj, rj = other
        dx, dy, dz, q = geometry(spots, xi, yi, zi, bi)
        hx, hy, hz = ax - bx, ay - by, az - bz
        wx, wy, wz = vx - ux, vy - uy, vz - uz
        dh = dx * hx + dy * hy + dz * hz
        ua = wx * ax + wy * ay + wz * az
        ub = wx * bx + wy * by + wz * bz
        coef = ci + cj
        along = q * (q * (ua * pj - ub * pi + (ri + rj)) - 4.0 * coef * dh)
        across = coef * (q * q)
        return along * dx + across * hx, along * dy + across * hy, along * dz + across * hz

    pairs(cnt, win, rows_at, body, places((geo, 4), (ga, 3), (wide, 6)), sums)

    def store(k, got):
        at = slice(128 * k, 128 * k + 128)
        gp = carry[0:3, at] + MU * got[0:3]
        gv = carry[3:6, at] + by_vel[0:3, at]
        if not final:
            gv = gv + DT * gp
            held = live_of(tab_i, k)[0:3]
            grad[0:3, at] = jnp.where(held, DT * gv, 0.0)
            grad[3:4, at] = jnp.zeros((1, 128), F32)
        else:
            grad[:, at] = jnp.zeros((4, 128), F32)
        new[0:3, at] = gp
        new[3:6, at] = gv
        new[6:8, at] = jnp.zeros((2, 128), F32)

    sums_to_own(cnt, sums, 3, cols, rows, tab_i, store)


def second_sweep(final, *ins):
    return call(
        functools.partial(second_kernel, final),
        "adjoint2",
        ins,
        (0, 1),
        (GRAD, OWN),
        (pltpu.VMEM((8, 4096), F32), pltpu.VMEM((1024, 8), F32)) + scratch(6, 3),
    )


def attributes(half):
    far = jnp.where(half == 0, 4.0, -1.0)
    tiles = [(0.0, float(b)) for b in range(4)] + [(-1.0, float(b)) for b in range(4)]
    tiles += [(1.0, float(b)) for b in range(4)] + [(0.0, far), (-1.0, far), (1.0, far), (0.0, 0.0)]
    zero = jnp.zeros((16,), F32)
    a = jnp.array([t[0] for t in tiles], F32)
    b = jnp.stack([jnp.asarray(t[1], F32) for t in tiles])
    return jnp.repeat(jnp.stack([a, b, zero, zero, zero, zero, b, zero]), 256, axis=1)


def per_device(nx, ny, positions, velocities, occupancy, cot_positions, cot_velocities):
    ring = 2 * nx
    flat = lambda a: a.reshape(3, 1024)
    slots = lax.broadcasted_iota(I32, (2, 2, 256), 2)
    live = (slots < occupancy[:, :, None]).astype(F32).reshape(1, 1024)
    zero = jnp.zeros((1, 1024), F32)
    state = jnp.concatenate(
        [flat(positions), flat(velocities), live, zero, flat(cot_positions), flat(cot_velocities), zero, zero], axis=0
    )
    gy_odd = lax.axis_index("gy") % 2
    column, half = mesh_to_logical(lax.axis_index("gx"), lax.axis_index("gy"))
    col_odd = column % 2

    def mesh_id(column, half):
        x, y = logical_to_mesh(column, half)
        return x * ny + y

    same = [(x * ny + y, mesh_id(2 * x + y % 2, y // 2)) for x in range(nx) for y in range(ny)]
    cross = [(x * ny + y, mesh_id(2 * x + 1 - y % 2, y // 2)) for x in range(nx) for y in range(ny)]

    def swap(value, odd, first, second):
        low, high = value[:, :512], value[:, 512:]
        one = lax.ppermute(jnp.where(odd == 0, low, high), ("gx", "gy"), first)
        two = lax.ppermute(jnp.where(odd == 0, high, low), ("gx", "gy"), second)
        return one, two

    def join(one, two, odd):
        return jnp.concatenate([jnp.where(odd == 0, one, two), jnp.where(odd == 0, two, one)], axis=1)

    state = join(*swap(state, gy_odd, same, cross), col_odd)
    grad_vel = state[11:14] + DT * state[8:11]
    grad = DT * state[6:7] * grad_vel
    carry = jnp.concatenate([state[8:11], grad_vel, jnp.zeros((2, 1024), F32)], axis=0)
    own = state[0:8]
    start = jnp.concatenate([own, grad, jnp.zeros((5, 1024), F32)], axis=0)
    attr_j = attributes(half)
    attr_i = attr_j[:, :1024]

    hal16 = halo(start, ring, 1)
    hal = hal16[0:8]
    grad, grad_h = start[8:12], hal16[8:12]
    tab_j, tab_i, cnt = plan(own, hal)
    history = []
    for step in range(STEPS):
        if step:
            hal = halo(own, ring, 0)
        mj, ic, win, rho, geo = density(cnt, own, hal, attr_j, attr_i, tab_j, tab_i)
        rho_h = halo(rho, ring, 2)
        before = own
        if step + 1 < STEPS:
            mc, cc, own = force(cnt, win, rho, rho_h, own, mj, geo, tab_j, tab_i)
        else:
            mc, cc = pressure_only(cnt, rho, rho_h, tab_j, tab_i)
        history.append((win, rho, mj, ic, geo, mc, cc, before))
    for step in reversed(range(STEPS)):
        win, rho, mj, ic, geo, mc, cc, state_at = history[step]
        mg, ga, part, by_vel = first_sweep(cnt, win, state_at, grad, grad_h, rho, mj, geo, mc, tab_j, tab_i)
        part_h = halo(part, ring, 2)
        grad, carry = second_sweep(
            step == 0, cnt, win, part, part_h, by_vel, carry, mj, ic, geo, mc, cc, mg, ga, tab_j, tab_i
        )
        if step:
            grad_h = halo(grad, ring, 3)
    back = lambda moves: [(d, s) for s, d in moves]
    result = join(*swap(carry, col_odd, back(same), back(cross)), gy_odd)
    return result[0:3].reshape(positions.shape), result[3:6].reshape(positions.shape)


def solution(mesh):
    spec = P(None, "gx", "gy", None)
    return jax.shard_map(
        functools.partial(per_device, mesh.shape["gx"], mesh.shape["gy"]),
        mesh=mesh,
        in_specs=(spec, spec, P("gx", "gy"), spec, spec),
        out_specs=(spec, spec),
        check_vma=False,
    )
```

```python
import functools

import jax
import jax.numpy as jnp
import numpy as np
from jax import lax
from jax.experimental import pallas as pl
from jax.experimental.pallas import tpu as pltpu
from jax.sharding import PartitionSpec as P

STEPS = 4
DT = 0.05
MU = 0.15
MESH = pl.DeviceIdType.MESH
F32 = jnp.float32
I32 = jnp.int32
NJ, NI = 32, 8
NK = 30
PAD = 64
NS = 128
REACH = 1.0001


def logical_to_mesh(column, half):
    y = column // 32
    s = column % 32
    s = s + (y % 2) * (31 - 2 * s)
    z = s // 4
    x = s % 4
    x = x + (z % 2) * (3 - 2 * x)
    return (y * 2 + x % 2) * 8 + z, (x // 2) * 2 + half


def mesh_to_logical(gx, gy):
    y = gx // 16
    z = gx % 8
    x = (gy // 2) * 2 + (gx // 8) % 2
    s = 4 * z + x + (z % 2) * (3 - 2 * x)
    return 32 * y + s + (y % 2) * (31 - 2 * s), gy % 2


def halo_kernel(ring, src, out, send_sem, recv_sem):
    column, half = mesh_to_logical(lax.axis_index("gx"), lax.axis_index("gy"))
    left, right, other = (column + ring - 1) % ring, (column + 1) % ring, 1 - half
    barrier = pltpu.get_barrier_semaphore()
    for who in ((left, half), (right, half), (left, other), (right, other), (column, other)):
        pl.semaphore_signal(barrier, inc=1, device_id=logical_to_mesh(*who), device_id_type=MESH)
    pl.semaphore_wait(barrier, 5)
    rim = pl.multiple_of(768 * other, 128)

    def copy(k, start, dest, n, who):
        return pltpu.make_async_remote_copy(
            src_ref=src.at[:, pl.ds(start, n)],
            dst_ref=out.at[:, pl.ds(dest, n)],
            send_sem=send_sem.at[k],
            recv_sem=recv_sem.at[k],
            device_id=logical_to_mesh(*who),
            device_id_type=MESH,
        )

    copies = [
        copy(0, rim, 2304, 256, (right, other)),
        copy(1, rim, 2560, 256, (left, other)),
        copy(2, 0, 0, 1024, (right, half)),
        copy(3, 0, 1024, 1024, (left, half)),
        copy(4, rim, 2048, 256, (column, other)),
    ]
    for c in copies:
        c.start()
    for c in copies:
        c.wait()


VM = pl.BlockSpec(memory_space=pltpu.VMEM)
SM = pl.BlockSpec(memory_space=pltpu.SMEM)


def halo(own, ring, cid):
    rows = own.shape[0]
    return pl.pallas_call(
        functools.partial(halo_kernel, ring),
        out_shape=jax.ShapeDtypeStruct((rows, 3072), F32),
        in_specs=[VM],
        out_specs=VM,
        scratch_shapes=[pltpu.SemaphoreType.DMA((5,)), pltpu.SemaphoreType.DMA((5,))],
        compiler_params=pltpu.CompilerParams(
            collective_id=cid, has_side_effects=True, vmem_limit_bytes=2 << 20
        ),
        name=f"halo{rows}",
    )(own)


def iota(shape, dim):
    return lax.broadcasted_iota(I32, shape, dim)


def dot_t(a, b):
    return lax.dot_general(a, b, (((1,), (1,)), ((), ())), preferred_element_type=F32)


def plan_kernel(own, hal, tab_j, tab_i, cnt, pre):
    sub = iota((NS, 128), 0)
    lane = iota((NS, 128), 1)
    upper = jnp.where(sub <= lane, 1.0, 0.0).astype(jnp.bfloat16)
    strict = jnp.where(lane < sub, 1.0, 0.0)

    def row(k):
        if k < NI:
            z = own[2:3, 128 * k : 128 * k + 128]
            live = own[6:7, 128 * k : 128 * k + 128] > 0.5
        else:
            s = 128 * (k - NI)
            z = hal[2:3, s : s + 128]
            live = hal[6:7, s : s + 128] > 0.5
        bucket = jnp.clip((z * 8.0).astype(I32), 0, NS - 1)
        return jnp.where(live, bucket, -1)

    carry = jnp.zeros((NS, 1), F32)
    total_i = carry
    for k in range(NK):
        hot = jnp.where(sub == row(k), 1.0, 0.0)
        count = jnp.dot(hot.astype(jnp.bfloat16), upper, preferred_element_type=F32)
        pre[:, 128 * k : 128 * k + 128] = count + carry - 1.0
        carry = carry + count[:, 127:128]
        if k == NI - 1:
            total_i = carry
    hi = lax.Precision.HIGHEST
    off_j = jnp.dot(strict, jnp.broadcast_to(carry, (NS, 128)), precision=hi, preferred_element_type=F32)
    off_i = jnp.dot(strict, jnp.broadcast_to(total_i, (NS, 128)), precision=hi, preferred_element_type=F32)

    def inverse(blocks, offset, nh, k, acc):
        b = row(k)
        rank = jnp.sum(
            jnp.where(sub == b, pre[:, 128 * k : 128 * k + 128] + offset, 0.0), axis=0, keepdims=True
        ).astype(I32)
        rank = jnp.where(b >= 0, rank, -128)
        high, low = rank >> 7, rank & 127
        eq = iota((nh, 128), 0) == high
        a = jnp.concatenate(
            [jnp.where(eq, iota((nh, 128), 1), 0), jnp.where(eq, k + 1, 0)], axis=0
        ).astype(F32).astype(jnp.bfloat16)
        hot = jnp.where(sub == low, 1.0, 0.0).astype(jnp.bfloat16)
        return acc + dot_t(a, hot), high, low

    acc = jnp.zeros((2 * NJ, 128), F32)
    for k in range(NK):
        acc, _, _ = inverse(NJ, off_j, NJ, k, acc)
    tab_j[0:NJ, :] = acc[0:NJ].astype(I32)
    tab_j[NJ : 2 * NJ, :] = acc[NJ:].astype(I32) - 1
    acc = jnp.zeros((2 * NI, 128), F32)
    for k in range(NI):
        acc, high, low = inverse(NI, off_i, NI, k, acc)
        tab_i[16 + k : 17 + k, :] = high
        tab_i[24 + k : 25 + k, :] = jnp.maximum(low, 0)
    tab_i[0:NI, :] = acc[0:NI].astype(I32)
    tab_i[NI : 2 * NI, :] = acc[NI:].astype(I32) - 1
    nj = jnp.sum(carry, axis=0, keepdims=True)
    ni = jnp.sum(total_i, axis=0, keepdims=True)
    at = iota((1, 128), 1)
    blocks_j = (nj + 127.0).astype(I32) >> 7
    groups_i = (ni + 31.0).astype(I32) >> 5
    cnt[...] = jnp.where(at == 0, blocks_j, groups_i)


def plan(own, hal):
    return pl.pallas_call(
        plan_kernel,
        out_shape=(
            jax.ShapeDtypeStruct((2 * NJ, 128), I32),
            jax.ShapeDtypeStruct((32, 128), I32),
            jax.ShapeDtypeStruct((1, 128), I32),
        ),
        in_specs=[VM] * 2,
        out_specs=(VM, VM, VM),
        scratch_shapes=[pltpu.VMEM((NS, 4096), F32)],
        compiler_params=pltpu.CompilerParams(vmem_limit_bytes=8 << 20),
        name="plan",
    )(own, hal)


def take(block, idx):
    return jnp.take_along_axis(block, idx, axis=1, mode="promise_in_bounds")


def gather(load, count, table, lane_row, blk_row):
    idx = jnp.broadcast_to(table[pl.ds(lane_row, 1), :], (8, 128))
    blk = jnp.broadcast_to(table[pl.ds(blk_row, 1), :], (8, 128))
    out = jnp.zeros((8, 128), F32)
    for k in range(count):
        out = jnp.where(blk == k, take(load(k), idx), out)
    return out


def spread(own, hal, stage, n):
    for k in range(NK):
        part = own[:, 128 * k : 128 * k + 128] if k < NI else hal[:, 128 * (k - NI) : 128 * (k - NI) + 128]
        for c in range(n):
            stage[NJ * c + k : NJ * c + k + 1, :] = part[c : c + 1]


def pick(stage, c, groups, idx, blk):
    sub = iota((8, 128), 0)
    out = jnp.zeros((8, 128), F32)
    for j in range(groups):
        part = stage[NJ * c + 8 * j : NJ * c + 8 * j + 8, :]
        out = jnp.where(blk == sub + 8 * j, take(part, idx), out)
    return jnp.sum(out, axis=0, keepdims=True)


def entry(table, lane_row, blk_row):
    idx = jnp.broadcast_to(table[pl.ds(lane_row, 1), :], (8, 128))
    return idx, jnp.broadcast_to(table[pl.ds(blk_row, 1), :], (8, 128))


def each_block(cnt, fill, together=8):
    def several(b, _):
        for n in range(together):
            fill(together * b + n, 0)
        return 0

    lax.fori_loop(0, (cnt[0, 0] + together - 1) >> (together.bit_length() - 1), several, 0)


def block(ref, m):
    return ref[:, pl.ds(pl.multiple_of(m * 128, 128), 128)]


def put(ref, m, value):
    ref[:, pl.ds(pl.multiple_of(m * 128, 128), 128)] = value


def columns(ref, k, rows):
    ref[128 * k : 128 * k + 128, :] = rows.T


def sums_to_own(cnt, sums, n_out, cols, rows, tab_i, store):
    def reduce(b, _):
        for n in range(4):
            at = pl.multiple_of(b * 512 + 128 * n, 128)
            for c in range(n_out):
                cols[pl.ds(at, 128), c : c + 1] = jnp.sum(sums[c, pl.ds(at, 128), :], axis=1, keepdims=True)
        for n in range(4):
            at = pl.multiple_of(b * 512 + 128 * n, 128)
            rows[:, pl.ds(at, 128)] = cols[pl.ds(at, 128), :].T
        return 0

    lax.fori_loop(0, (cnt[0, 1] + 15) >> 4, reduce, 0)
    load = lambda m: rows[:, 128 * m : 128 * m + 128]
    for k in range(NI):
        store(k, gather(load, NI, tab_i, 24 + k, 16 + k))


def broadcast_columns(cnt, channels, sums, n_out):
    def one(b, _):
        at = pl.multiple_of(b * 128, 128)
        for ref, c, wide, n in channels:
            wide[n, pl.ds(at, 128), :] = jnp.broadcast_to(ref[pl.ds(at, 128), c : c + 1], (128, 128))
        for c in range(n_out):
            sums[c, pl.ds(at, 128), :] = jnp.zeros((128, 128), F32)
        return 0

    lax.fori_loop(0, (cnt[0, 1] + 3) >> 2, one, 0)


def pairs(cnt, win, rows, body, mine, sums, size=32):
    def each(m, _):
        picked = rows(m)
        first = win[m, 0]

        def chunk(n, _):
            at = pl.multiple_of((first + (size // 8) * n) * 8, 8)
            terms = body(picked, *[wide[c, pl.ds(at, size), :] for wide, c in mine])
            for c, term in enumerate(terms):
                sums[c, pl.ds(at, size), :] += term
            return 0

        lax.fori_loop(0, (win[m, 1] + (size - 1)) >> (size.bit_length() - 1), chunk, 0)
        return 0

    lax.fori_loop(0, cnt[0, 0], each, 0)


def places(*refs):
    return [(ref, c) for ref, count in refs for c in range(count)]


def row_of(ref, c, m):
    return ref[c : c + 1, pl.ds(pl.multiple_of(m * 128, 128), 128)]


def spot(mj, m):
    return [row_of(mj, c, m) for c in GEO]


def geometry(spots, xi, yi, zi, bi):
    xj, yj, zj, bj = [jnp.broadcast_to(r, xi.shape) for r in spots]
    dx, dy, dz, db = xj - xi, yj - yi, zj - zi, bj - bi
    top = jnp.minimum(2.0 - db * db, 1.0)
    q = jnp.maximum(top - (dx * dx + dy * dy + dz * dz), 0.0)
    return dx, dy, dz, q


GEO = (0, 1, 2, 6)


def live_of(tab_i, k):
    return jnp.broadcast_to(tab_i[16 + k : 17 + k, :], (8, 128)) >= 0


def density_kernel(cnt, own, hal, attr_j, attr_i, tab_j, tab_i, mj, ic, win, rho, geo, cols, rows, zlo, zhi, win_s, sem, stage, sums):
    body6 = iota((8, 128), 0) < 6
    for k in range(NK):
        part = own[0:8, 128 * k : 128 * k + 128] if k < NI else hal[0:8, 128 * (k - NI) : 128 * (k - NI) + 128]
        stage[:, 128 * k : 128 * k + 128] = jnp.where(body6, part, 0.0) + attr_j[:, 128 * k : 128 * k + 128]
    load = lambda k: stage[:, 128 * k : 128 * k + 128]
    zlo[...] = jnp.full((NJ, 128), 1e30, F32)
    zhi[...] = jnp.full((NJ, 128), -1e30, F32)

    def fill(m, _):
        got = gather(load, NK, tab_j, m, NJ + m)
        held = tab_j[pl.ds(NJ + m, 1), :] >= 0
        put(mj, m, jnp.where((iota((8, 128), 0) == 6) & ~held, 1000.0, got))
        zlo[pl.ds(m, 1), :] = jnp.where(held, got[2:3], 1e30)
        zhi[pl.ds(m, 1), :] = jnp.where(held, got[2:3], -1e30)
        return 0

    each_block(cnt, fill, 4)
    body6 = iota((8, 128), 0) < 6

    def load_i(k):
        at = slice(128 * k, 128 * k + 128)
        return jnp.where(body6, own[:, at], 0.0) + attr_i[:, at]

    z_rows = []
    for k in range(NI):
        got = gather(load_i, NI, tab_i, k, NI + k)
        columns(ic, k, got)
        z_rows.append(got[2:3])
    low = jnp.min(zlo[...], axis=1, keepdims=True) - REACH
    high = jnp.max(zhi[...], axis=1, keepdims=True) + REACH
    first = jnp.full((NJ, 128), 4096, I32)
    last = jnp.zeros((NJ, 128), I32)
    for k in range(NI):
        held = tab_i[NI + k : NI + k + 1, :] >= 0
        meets = (z_rows[k] > low) & (z_rows[k] < high) & held
        at = iota((NJ, 128), 1) + 128 * k
        first = jnp.minimum(first, jnp.where(meets, at, 4096))
        last = jnp.maximum(last, jnp.where(meets, at + 1, 0))
    first = jnp.min(first.astype(F32), axis=1, keepdims=True).astype(I32) >> 3
    last = jnp.max(last.astype(F32), axis=1, keepdims=True).astype(I32)
    chunks = jnp.maximum(last - 8 * first, 0)
    windows = jnp.where(iota((NJ, 128), 1) == 0, first, chunks)
    win[...] = windows
    copy = pltpu.make_async_copy(win, win_s, sem)
    copy.start()
    broadcast_columns(cnt, [(ic, c, geo, n) for n, c in enumerate(GEO)], sums, 1)
    copy.wait()

    def body(spots, *mine):
        _, _, _, q = geometry(spots, *mine)
        return (q * q * q,)

    pairs(cnt, win_s, lambda m: spot(mj, m), body, places((geo, 4)), sums, 64)

    def store(k, got):
        rho[:, 128 * k : 128 * k + 128] = MU * got[0:1]

    sums_to_own(cnt, sums, 1, cols, rows, tab_i, store)


def call(kernel, name, ins, smem, outs, scratch=()):
    specs = [SM if i in smem else VM for i in range(len(ins))]
    return pl.pallas_call(
        kernel,
        out_shape=tuple(jax.ShapeDtypeStruct(s, t) for s, t in outs),
        in_specs=specs,
        out_specs=tuple(VM for _ in outs),
        scratch_shapes=list(scratch),
        compiler_params=pltpu.CompilerParams(vmem_limit_bytes=12 << 20),
        name=name,
    )(*ins)


def scratch(n_in, n_out):
    return (
        pltpu.VMEM((1024, 8), F32),
        pltpu.VMEM((8, 1024), F32),
        pltpu.VMEM((8 * NJ, 128), F32),
        pltpu.VMEM((n_in, 1024 + PAD, 128), F32),
        pltpu.VMEM((n_out, 1024 + PAD, 128), F32),
    )


COLS = ((1024, 8), F32)
OWN = ((8, 1024), F32)
ROW = ((1, 1024), F32)


def lanes(n):
    return ((n, 1024 + PAD, 128), F32)


GRAD = ((4, 1024), F32)
WIDE = ((8, 4096), F32)


def density(cnt, own, hal, attr_j, attr_i, tab_j, tab_i):
    return call(
        density_kernel,
        "density",
        (cnt, own, hal, attr_j, attr_i, tab_j, tab_i),
        (0,),
        (WIDE, COLS, ((NJ, 128), I32), ROW, lanes(4)),
        (
            pltpu.VMEM((1024, 8), F32),
            pltpu.VMEM((8, 1024), F32),
            pltpu.VMEM((NJ, 128), F32),
            pltpu.VMEM((NJ, 128), F32),
            pltpu.SMEM((NJ, 128), I32),
            pltpu.SemaphoreType.DMA,
            pltpu.VMEM((8, 4096), F32),
            pltpu.VMEM((1, 1024 + PAD, 128), F32),
        ),
    )


def pressure(rho_row, held):
    padded = jnp.where(held, rho_row, 1.0)
    inverse = 1.0 / padded
    return 24.0 * (padded - 1.0) * inverse * inverse, 3.0 * inverse


def pressure_tables(cnt, rho, rho_h, tab_j, tab_i, mc, cc, stage):
    spread(rho, rho_h, stage, 1)
    row8 = iota((8, 128), 0)

    def table(got, held):
        coef, inv = pressure(got, held)
        return jnp.where(row8 == 0, coef, jnp.where(row8 == 1, inv, 0.0))

    def fill(m, _):
        idx, blk = entry(tab_j, m, NJ + m)
        put(mc, m, table(pick(stage, 0, 4, idx, blk), tab_j[pl.ds(NJ + m, 1), :] >= 0))
        return 0

    each_block(cnt, fill)
    for k in range(NI):
        idx, blk = entry(tab_i, k, NI + k)
        columns(cc, k, table(pick(stage, 0, 1, idx, blk), tab_i[NI + k : NI + k + 1, :] >= 0))


def force_kernel(cnt, win, rho, rho_h, own, mj, geo, tab_j, tab_i, mc, cc, new, cols, rows, stage, wide, sums):
    pressure_tables(cnt, rho, rho_h, tab_j, tab_i, mc, cc, stage)
    broadcast_columns(cnt, [(cc, 0, wide, 0)], sums, 4)

    def rows_at(m):
        return spot(mj, m), [row_of(mj, c, m) for c in (3, 4, 5)], row_of(mc, 0, m), row_of(mc, 1, m) * (1.0 / 6.0)

    def body(other, xi, yi, zi, bi, ci):
        spots, (vx, vy, vz), cj, pj = other
        dx, dy, dz, q = geometry(spots, xi, yi, zi, bi)
        q2 = q * q
        push = (ci + cj) * q2
        drag = q2 * q * pj
        return drag * vx - push * dx, drag * vy - push * dy, drag * vz - push * dz, drag

    pairs(cnt, win, rows_at, body, places((geo, 4), (wide, 1)), sums, 32)


    def store(k, got):
        at = slice(128 * k, 128 * k + 128)
        v = [own[3 + c : 4 + c, at] for c in range(3)]
        v = [v[c] + (DT * MU) * (got[c : c + 1] - v[c] * got[3:4]) for c in range(3)]
        x = [own[c : c + 1, at] + DT * v[c] for c in range(3)]
        new[0:3, at] = jnp.concatenate(x, axis=0)
        new[3:6, at] = jnp.concatenate(v, axis=0)
        new[6:8, at] = own[6:8, at]

    sums_to_own(cnt, sums, 4, cols, rows, tab_i, store)


def force(cnt, win, rho, rho_h, own, mj, geo, tab_j, tab_i):
    return call(
        force_kernel,
        "force",
        (cnt, win, rho, rho_h, own, mj, geo, tab_j, tab_i),
        (0, 1),
        (WIDE, COLS, OWN),
        scratch(1, 4),
    )


def first_kernel(cnt, win, own, grad, grad_h, rho, mj, geo, mc, tab_j, tab_i, mg, ga, out, by_vel, gc, cols, rows, stage, wide, sums):
    spread(grad, grad_h, stage, 3)
    none = jnp.zeros((5, 128), F32)

    def fill(m, _):
        idx, blk = entry(tab_j, m, NJ + m)
        got = [pick(stage, c, 4, idx, blk) for c in range(3)]
        put(mg, m, jnp.concatenate(got + [none], axis=0))
        return 0

    each_block(cnt, fill)
    for k in range(NI):
        idx, blk = entry(tab_i, k, NI + k)
        got = [pick(stage, c, 1, idx, blk) for c in range(3)]
        columns(gc, k, jnp.concatenate(got + [none], axis=0))
    broadcast_columns(cnt, [(gc, c, ga, c) for c in range(3)], sums, 6)

    def rows_at(m):
        g = [row_of(mg, c, m) for c in range(3)]
        v = [row_of(mj, c, m) for c in (3, 4, 5)]
        return spot(mj, m), g, v[0] * g[0] + v[1] * g[1] + v[2] * g[2], row_of(mc, 1, m)

    def body(other, xi, yi, zi, bi, ax, ay, az):
        spots, (bx, by, bz), work, pj = other
        dx, dy, dz, q = geometry(spots, xi, yi, zi, bi)
        q2 = q * q
        q3 = q2 * q
        dh = dx * (ax - bx) + dy * (ay - by) + dz * (az - bz)
        return q2 * dh, q3 * work, q3 * pj, q3 * bx, q3 * by, q3 * bz

    pairs(cnt, win, rows_at, body, places((geo, 4), (ga, 3)), sums, 32)

    def store(k, got):
        at = slice(128 * k, 128 * k + 128)
        held = live_of(tab_i, k)[0:1]
        p = jnp.where(held, rho[0:1, at], 1.0)
        inv = 1.0 / p
        inv2 = inv * inv
        by_coef = (-6.0 * MU) * got[0:1]
        drag = got[1:2] - (own[3:4, at] * got[3:4] + own[4:5, at] * got[4:5] + own[5:6, at] * got[5:6])
        by_pad = (0.5 * MU) * inv2 * drag
        g_rho = by_coef * (4.0 * inv2 - 8.0 * (p - 1.0) * inv2 * inv) + by_pad
        out[0:1, at] = jnp.where(held, 6.0 * g_rho, 0.0)
        by_vel[0:3, at] = (-0.5 * MU) * (grad[0:3, at] * (got[2:3] * (1.0 / 3.0)) - inv * got[3:6])
        by_vel[3:4, at] = jnp.zeros((1, 128), F32)

    sums_to_own(cnt, sums, 6, cols, rows, tab_i, store)


def first_with_pressure(cnt, win, rho_h, own, grad, grad_h, rho, mj, geo, tab_j, tab_i, mg, ga, out, by_vel, mc, cc, gc, cols, rows, stage, wide, sums):
    pressure_tables(cnt, rho, rho_h, tab_j, tab_i, mc, cc, stage)
    first_kernel(
        cnt, win, own, grad, grad_h, rho, mj, geo, mc, tab_j, tab_i, mg, ga, out, by_vel, gc, cols, rows, stage, wide, sums
    )


def first_sweep(kernel, *ins):
    return call(
        kernel,
        "adjoint1",
        ins,
        (0, 1),
        (WIDE, lanes(3), ROW, GRAD) + ((WIDE, COLS) if kernel is first_with_pressure else ()),
        (pltpu.VMEM((1024, 8), F32),) + scratch(1, 6),
    )


def second_kernel(final, cnt, win, part, part_h, by_vel, carry, mj, ic, geo, mc, cc, mg, ga, tab_j, tab_i, grad, new, mp, pc, cols, rows, stage, wide, sums):
    spread(part, part_h, stage, 1)

    def fill(m, _):
        idx, blk = entry(tab_j, m, NJ + m)
        put(mp, m, jnp.broadcast_to(pick(stage, 0, 4, idx, blk), (8, 128)))
        return 0

    each_block(cnt, fill)
    for k in range(NI):
        idx, blk = entry(tab_i, k, NI + k)
        columns(pc, k, jnp.broadcast_to(pick(stage, 0, 1, idx, blk), (8, 128)))
    taken = [(ic, 3), (ic, 4), (ic, 5), (cc, 0), (cc, 1), (pc, 0)]
    broadcast_columns(cnt, [(ref, c, wide, n) for n, (ref, c) in enumerate(taken)], sums, 3)

    def rows_at(m):
        v = [row_of(mj, c, m) for c in (3, 4, 5)]
        g = [row_of(mg, c, m) for c in range(3)]
        return spot(mj, m), v, g, row_of(mc, 0, m), row_of(mc, 1, m), row_of(mp, 0, m)

    def body(other, xi, yi, zi, bi, ax, ay, az, ux, uy, uz, ci, pi, ri):
        spots, (vx, vy, vz), (bx, by, bz), cj, pj, rj = other
        dx, dy, dz, q = geometry(spots, xi, yi, zi, bi)
        hx, hy, hz = ax - bx, ay - by, az - bz
        wx, wy, wz = vx - ux, vy - uy, vz - uz
        dh = dx * hx + dy * hy + dz * hz
        ua = wx * ax + wy * ay + wz * az
        ub = wx * bx + wy * by + wz * bz
        coef = ci + cj
        along = q * (q * (ua * pj - ub * pi + (ri + rj)) - 4.0 * coef * dh)
        across = coef * (q * q)
        return along * dx + across * hx, along * dy + across * hy, along * dz + across * hz

    pairs(cnt, win, rows_at, body, places((geo, 4), (ga, 3), (wide, 6)), sums)

    def store(k, got):
        at = slice(128 * k, 128 * k + 128)
        gp = carry[0:3, at] + MU * got[0:3]
        gv = carry[3:6, at] + by_vel[0:3, at]
        if not final:
            gv = gv + DT * gp
            held = live_of(tab_i, k)[0:3]
            grad[0:3, at] = jnp.where(held, DT * gv, 0.0)
            grad[3:4, at] = jnp.zeros((1, 128), F32)
        else:
            grad[:, at] = jnp.zeros((4, 128), F32)
        new[0:3, at] = gp
        new[3:6, at] = gv
        new[6:8, at] = jnp.zeros((2, 128), F32)

    sums_to_own(cnt, sums, 3, cols, rows, tab_i, store)


def second_sweep(final, *ins):
    return call(
        functools.partial(second_kernel, final),
        "adjoint2",
        ins,
        (0, 1),
        (GRAD, OWN),
        (pltpu.VMEM((8, 4096), F32), pltpu.VMEM((1024, 8), F32)) + scratch(6, 3),
    )


def attributes(far):
    tiles = [(a, float(b)) for a in (0.0, -1.0, 1.0) for b in range(4)]
    tiles += [(0.0, far), (-1.0, far), (1.0, far), (0.0, 0.0)]
    table = np.array([[a, b, 0, 0, 0, 0, b, 0] for a, b in tiles], np.float32).T
    return jnp.asarray(np.repeat(table, 256, axis=1))


def per_device(nx, ny, positions, velocities, occupancy, cot_positions, cot_velocities):
    ring = 2 * nx
    slots = lax.broadcasted_iota(I32, (1, 2, 2, 256), 3)
    live = (slots < occupancy[None, :, :, None]).astype(F32)
    zero = jnp.zeros((1, 2, 2, 256), F32)
    state = jnp.concatenate(
        [positions, velocities, live, zero, cot_positions, cot_velocities, zero, zero], axis=0
    ).reshape(16, 1024)
    gy_odd = lax.axis_index("gy") % 2
    column, half = mesh_to_logical(lax.axis_index("gx"), lax.axis_index("gy"))
    col_odd = column % 2

    def mesh_id(column, half):
        x, y = logical_to_mesh(column, half)
        return x * ny + y

    same = [(x * ny + y, mesh_id(2 * x + y % 2, y // 2)) for x in range(nx) for y in range(ny)]
    cross = [(x * ny + y, mesh_id(2 * x + 1 - y % 2, y // 2)) for x in range(nx) for y in range(ny)]

    def swap(value, odd, first, second):
        low, high = value[:, :512], value[:, 512:]
        one = lax.ppermute(jnp.where(odd == 0, low, high), ("gx", "gy"), first)
        two = lax.ppermute(jnp.where(odd == 0, high, low), ("gx", "gy"), second)
        return one, two

    def join(one, two, odd):
        return jnp.concatenate([jnp.where(odd == 0, one, two), jnp.where(odd == 0, two, one)], axis=1)

    state = join(*swap(state, gy_odd, same, cross), col_odd)
    grad_vel = state[11:14] + DT * state[8:11]
    grad = DT * state[6:7] * grad_vel
    carry = jnp.concatenate([state[8:11], grad_vel, jnp.zeros((2, 1024), F32)], axis=0)
    own = state[0:8]
    start = jnp.concatenate([own, grad, jnp.zeros((5, 1024), F32)], axis=0)
    attr_j = jnp.where(half == 0, attributes(4.0), attributes(-1.0))
    attr_i = attr_j[:, :1024]

    hal16 = halo(start, ring, 1)
    hal = hal16[0:8]
    grad, grad_h = start[8:12], hal16[8:12]
    tab_j, tab_i, cnt = plan(own, hal)
    history = []
    for step in range(STEPS):
        if step:
            hal = halo(own, ring, 0)
        mj, ic, win, rho, geo = density(cnt, own, hal, attr_j, attr_i, tab_j, tab_i)
        rho_h = halo(rho, ring, 2)
        before = own
        if step + 1 < STEPS:
            mc, cc, own = force(cnt, win, rho, rho_h, own, mj, geo, tab_j, tab_i)
        else:
            mc = cc = None
        history.append((win, rho, mj, ic, geo, mc, cc, before))
    for step in reversed(range(STEPS)):
        win, rho, mj, ic, geo, mc, cc, state_at = history[step]
        if mc is None:
            mg, ga, part, by_vel, mc, cc = first_sweep(
                first_with_pressure, cnt, win, rho_h, state_at, grad, grad_h, rho, mj, geo, tab_j, tab_i
            )
        else:
            mg, ga, part, by_vel = first_sweep(
                first_kernel, cnt, win, state_at, grad, grad_h, rho, mj, geo, mc, tab_j, tab_i
            )
        part_h = halo(part, ring, 2)
        grad, carry = second_sweep(
            step == 0, cnt, win, part, part_h, by_vel, carry, mj, ic, geo, mc, cc, mg, ga, tab_j, tab_i
        )
        if step:
            grad_h = halo(grad, ring, 3)
    back = lambda moves: [(d, s) for s, d in moves]
    result = join(*swap(carry, col_odd, back(same), back(cross)), gy_odd)
    result = result[0:6].reshape((6,) + positions.shape[1:])
    return result[0:3], result[3:6]


def solution(mesh):
    spec = P(None, "gx", "gy", None)
    return jax.shard_map(
        functools.partial(per_device, mesh.shape["gx"], mesh.shape["gy"]),
        mesh=mesh,
        in_specs=(spec, spec, P("gx", "gy"), spec, spec),
        out_specs=(spec, spec),
        check_vma=False,
    )
```
